32 devices in a mesh: group: 4 (over z), tensor: 8 (over y, x, core).
Axes of the slice: x: 2, y: 2, z: 4, core: 2. Of those that a mesh axis runs over, the one named last changes fastest.
Arguments:
- key_value_cache: bfloat16 [256, 1024, 256], P(('group', 'tensor')), may hold values from -8 to 8
- queries: bfloat16 [32, 48, 128], P('group'), may hold values from -200 to 200
- fresh_key_value: bfloat16 [32, 8, 256], P('group'), may hold values from -6 to 6
- lengths: int32 [32], P('group'), may hold values from 2 to 1023
- residual: bfloat16 [32, 6144], P('group'), may hold values from -100 to 100
- norm_gain: float32 [6144], replicated, may hold values from 0.1 to 1.9
- router_weight: bfloat16 [6144, 8], replicated, may hold values from -0.078125 to 0.078125
- routing: int32 [32, 2], P('group'), may hold values from 0 to 7, all different within a row
- expert_gate: bfloat16 [8, 6144, 8192], P(None, 'group', 'tensor'), may hold values from -0.078125 to 0.078125
- expert_up: bfloat16 [8, 6144, 8192], P(None, 'group', 'tensor'), may hold values from -0.078125 to 0.078125
Outputs:
- updated: bfloat16 [32, 6144], P('group')
- expert_hidden: bfloat16 [32, 2, 8192], P('group', None, 'tensor')
- new_cache: bfloat16 [32, 8, 1024, 256], P('group', None, 'tensor')
The draws below stay inside these ranges and needn't reach their ends.
Inputs may be any that keep to these rules, and one draw needn't show every extreme that they name: Slot lengths[s] of sequence s receives its new token. `routing`: A token's two experts differ.
All inputs are finite; a program needn't handle non-finite values.
Results may differ from the reference program's by a relative error of at most 0.028.
Values may be sent and summed in bfloat16 or wider, within the bound.
A program may use at most 128 MiB of HBM per device.

```python
import math
import jax
import jax.numpy as jnp
from jax import lax

D = 6144
QUERY_HEADS = 48
KEY_VALUE_HEADS = 8
HEAD_DIM = 128
EXPERTS = 8
TOPK = 2
FF_WIN = 8192
CONTEXT_SLOTS = 1024
SEQUENCE_TOTAL = 32


def starting_cache(key):
    cache_random_key = jax.random.fold_in(key, 7)
    return jnp.clip(jax.random.normal(cache_random_key, (SEQUENCE_TOTAL * KEY_VALUE_HEADS, CONTEXT_SLOTS, 2 * HEAD_DIM), jnp.float32), -6.0, 6.0)


def draw_key_value_cache(key, part):
    cache_layout_grid = starting_cache(key)
    return cache_layout_grid.astype(jnp.bfloat16)


def draw_queries(key, part):
    query_group_width = QUERY_HEADS // KEY_VALUE_HEADS
    query_vectors = jnp.clip(jax.random.normal(jax.random.fold_in(key, 21), (SEQUENCE_TOTAL, KEY_VALUE_HEADS, query_group_width, HEAD_DIM), jnp.float32), -4.0, 4.0)
    return query_vectors.reshape(SEQUENCE_TOTAL, QUERY_HEADS, HEAD_DIM).astype(jnp.bfloat16)


def draw_residual(key, part):
    base_key = jax.random.fold_in(key, 31)
    row_key = jax.random.fold_in(key, 32)
    column_key = jax.random.fold_in(key, 33)
    values = jnp.clip(jax.random.normal(base_key, (SEQUENCE_TOTAL, D), jnp.float32), -4.0, 4.0)
    row_scale = jnp.exp(jax.random.uniform(row_key, (SEQUENCE_TOTAL, 1), jnp.float32, jnp.log(0.4), jnp.log(4.0)))
    column_scale = jnp.exp(jax.random.uniform(column_key, (1, D), jnp.float32, jnp.log(0.4), jnp.log(4.0)))
    return (values * row_scale * column_scale).astype(jnp.bfloat16)


def touch_ends(values, rng, least, high):
    dims = values.shape
    spot = [jax.random.randint(jax.random.fold_in(rng, axis), (), 0, dims[axis]) for axis in range(len(dims))]
    values = values.at[tuple(spot)].set(least)
    longest = dims.index(max(dims))
    spot[longest] = (spot[longest] + 1) % dims[longest]
    return values.at[tuple(spot)].set(high)


def shard_levels(rng, shape, pieces, smallest, high):
    level, own = 1.0, jax.random.fold_in(rng, 6)
    for position, shards_of in pieces:
        heights = jnp.exp(jax.random.uniform(jax.random.fold_in(own, position), (shards_of,), jnp.float32, smallest / len(pieces), high / len(pieces)))
        level = level * jnp.repeat(heights, shape[position] // shards_of).reshape([-1 if axis == position else 1 for axis in range(len(shape))])
    return level


def picks_of(key, rows, amount, top, lift):
    sequence = jax.random.permutation(jax.random.fold_in(key, 1), amount)
    boost = sequence
    for power in range(3):
        boost = boost * boost // amount
    boost = boost * lift // amount
    tickets = jax.random.randint(jax.random.fold_in(key, 2), (rows, amount), 0, 4096) + boost
    holders = jax.random.permutation(jax.random.fold_in(key, 3), rows)[jnp.arange(amount) % rows]
    tickets = jnp.where(jnp.arange(rows)[:, None] == holders[None, :], 1 << 14, tickets)
    merit = tickets * amount + jnp.arange(amount)
    return lax.top_k(merit.astype(jnp.int32), top)[1].astype(jnp.int32)


def scatter_about(key, extent, scale, limit, shards=(), kind=jnp.bfloat16):
    loudness = shard_levels(key, extent, shards, -0.22, 0.18) if shards else 1.0
    values = jax.random.normal(key, extent, jnp.float32) * scale * loudness
    return jnp.minimum(jnp.maximum(values, -limit), limit).astype(kind)


def setup_inputs(seed: int = 0) -> dict:
    key_of = jax.random.split(jax.random.key(seed), 11)
    return {
        "key_value_cache": draw_key_value_cache(jax.random.fold_in(key_of[10], 71), 0),
        "queries": draw_queries(jax.random.fold_in(key_of[10], 71), 0),
        "fresh_key_value": scatter_about(key_of[2], (SEQUENCE_TOTAL, KEY_VALUE_HEADS, 2 * HEAD_DIM), 1.0, 6.0, ((0, 4),)),
        "lengths": touch_ends(jax.random.randint(key_of[3], (SEQUENCE_TOTAL,), 2, CONTEXT_SLOTS), jax.random.fold_in(key_of[3], 1), 2, CONTEXT_SLOTS - 1).astype(jnp.int32),
        "residual": draw_residual(jax.random.fold_in(key_of[10], 71), 0),
        "norm_gain": jnp.clip(1.0 + 0.18 * jax.random.normal(key_of[5], (D,), jnp.float32), 0.1, 1.9),
        "router_weight": scatter_about(key_of[6], (D, EXPERTS), D ** -0.5, 0.078125),
        "routing": picks_of(key_of[7], SEQUENCE_TOTAL, EXPERTS, TOPK, 2048),
        "expert_gate": scatter_about(key_of[8], (EXPERTS, D, FF_WIN), D ** -0.5, 0.078125, ((1, 4), (2, 8))),
        "expert_up": scatter_about(key_of[9], (EXPERTS, D, FF_WIN), D ** -0.5, 0.078125, ((1, 4), (2, 8))),
    }


def reference(key_value_cache, queries, fresh_key_value, lengths, residual, norm_gain, router_weight, routing, expert_gate, expert_up):
    query_group_width = QUERY_HEADS // KEY_VALUE_HEADS
    cache_layout_grid = key_value_cache.reshape(SEQUENCE_TOTAL, KEY_VALUE_HEADS, CONTEXT_SLOTS, 2 * HEAD_DIM)
    key_rows = cache_layout_grid[..., :HEAD_DIM].astype(jnp.float32)
    value_rows = cache_layout_grid[..., HEAD_DIM:].astype(jnp.float32)
    query_vectors = queries.reshape(SEQUENCE_TOTAL, KEY_VALUE_HEADS, query_group_width, HEAD_DIM).astype(jnp.float32)
    score_scale = 1.0 / math.sqrt(HEAD_DIM)
    scores = jnp.einsum('sngd,sntd->sngt', query_vectors, key_rows, precision=lax.Precision.HIGHEST) * score_scale
    own_key = fresh_key_value[..., :HEAD_DIM].astype(jnp.float32)
    own_value = fresh_key_value[..., HEAD_DIM:].astype(jnp.float32)
    own_score = jnp.einsum('sngd,snd->sng', query_vectors, own_key, precision=lax.Precision.HIGHEST) * score_scale
    visible = jnp.arange(CONTEXT_SLOTS, dtype=jnp.int32)[None, None, None, :] < lengths[:, None, None, None]
    peak = jnp.maximum(lax.optimization_barrier(jnp.max(jnp.where(visible, scores, -jnp.inf), -1)), own_score)
    attention_weights = jnp.where(visible, jnp.exp(scores - peak[..., None]), 0.0)
    own_weight = jnp.exp(own_score - peak)
    denominator = lax.optimization_barrier(jnp.sum(attention_weights, -1)) + own_weight
    rounded = lax.optimization_barrier(attention_weights.astype(jnp.bfloat16)).astype(jnp.float32)
    own_rounded = lax.optimization_barrier(own_weight.astype(jnp.bfloat16)).astype(jnp.float32)
    weighted = jnp.einsum('sngt,sntd->sngd', rounded, value_rows, precision=lax.Precision.HIGHEST)
    weighted = weighted + own_rounded[..., None] * own_value[:, :, None, :]
    attention = (weighted / denominator[..., None]).reshape(SEQUENCE_TOTAL, D)
    updated = (residual.astype(jnp.float32) + attention).astype(jnp.bfloat16)
    stream = updated.astype(jnp.float32)
    normed = (stream * lax.rsqrt(lax.optimization_barrier(jnp.mean(stream * stream, -1, keepdims=True)) + 1e-05) * norm_gain).astype(jnp.bfloat16)
    logits = jnp.dot(normed, router_weight, preferred_element_type=jnp.float32)
    chosen_mask = routing[:, :, None] == jnp.arange(EXPERTS, dtype=jnp.int32)[None, None, :]
    chosen_logits = lax.optimization_barrier(jnp.sum(jnp.where(chosen_mask, logits[:, None, :], 0.0), -1))
    gate_weights = jax.nn.sigmoid(chosen_logits - chosen_logits[:, ::-1])

    def expert_pass(weight_pair):
        gate_part = jnp.dot(normed, weight_pair[0], preferred_element_type=jnp.float32)
        up_part = jnp.dot(normed, weight_pair[1], preferred_element_type=jnp.float32)
        return jnp.stack((gate_part, up_part), 1)
    every_expert = lax.map(expert_pass, (expert_gate, expert_up))
    every_expert = jnp.transpose(every_expert, (1, 0, 2, 3))
    picked = lax.optimization_barrier(jnp.sum(jnp.where(chosen_mask[:, :, :, None, None], every_expert[:, None], 0.0), 2))
    expert_hidden = (gate_weights[:, :, None] * jax.nn.silu(picked[:, :, 0]) * picked[:, :, 1]).astype(jnp.bfloat16)
    new_slot = jnp.arange(CONTEXT_SLOTS, dtype=jnp.int32)[None, None, :, None] == lengths[:, None, None, None]
    new_cache = jnp.where(new_slot, fresh_key_value[:, :, None, :], cache_layout_grid)
    return (updated, expert_hidden, new_cache)
```

```python
import functools
import math

import jax
import jax.numpy as jnp
from jax import lax
from jax.experimental import pallas as pl
from jax.experimental.pallas import tpu as pltpu
from jax.sharding import PartitionSpec as P

MESH = pl.DeviceIdType.MESH
LANES = 128
NT = (((1,), (1,)), ((), ()))


def flip(rank, bits, count):
    out, step = rank, 1
    while step < count:
        if bits & step:
            out = out + step * (1 - 2 * (rank // step % 2))
        step *= 2
    return out


def swapped(bits, count):
    if count < 8 or (bits >> 1) % 2 == (bits >> 2) % 2:
        return bits
    return bits ^ 6


def kernel(
    n_t,
    n_g,
    cache_hbm,
    queries_hbm,
    fresh_hbm,
    lengths_hbm,
    residual_hbm,
    gain_hbm,
    router_hbm,
    routing_hbm,
    gate_hbm,
    up_hbm,
    updated_ref,
    hidden_ref,
    arrived,
    cache_v,
    queries_ref,
    fresh_ref,
    fresh_rows,
    lengths_ref,
    residual_ref,
    gain_ref,
    router_ref,
    routing_ref,
    gate_v,
    up_v,
    heads_b,
    heads_v,
    normed_v,
    x_send,
    x_recv,
    picked,
    p_send,
    p_recv,
    load_sem,
    small_sem,
    gate_sem,
    up_sem,
    a_send_sem,
    a_recv_sem,
    b_send_sem,
    b_recv_sem,
    h_send_sem,
    h_recv_sem,
    x_send_sem,
    x_recv_sem,
    p_send_sem,
    p_recv_sem,
):
    tensor = lax.axis_index("tensor")
    group = lax.axis_index("group")
    pairs, slots, width = cache_v.shape
    head = width // 2
    span = slots // n_t
    first = max(1, pairs // 2)
    seqs, q_heads, _ = queries_ref.shape
    kv_heads = fresh_ref.shape[1]
    per = q_heads // kv_heads
    experts = gate_v.shape[0]
    depth = gate_v.shape[1]
    columns = residual_ref.shape[1]
    shares = heads_v.shape[1]

    load = pltpu.make_async_copy(cache_hbm, cache_v, load_sem)
    load.start()
    small = [
        pltpu.make_async_copy(src, dst, small_sem.at[i])
        for i, (src, dst) in enumerate(
            (
                (queries_hbm, queries_ref),
                (fresh_hbm, fresh_ref),
                (lengths_hbm, lengths_ref),
                (routing_hbm, routing_ref),
                (residual_hbm, residual_ref),
                (gain_hbm, gain_ref),
                (router_hbm, router_ref),
            )
        )
    ]

    odd = tensor % 2
    t_peers = [
        (1 - odd) * flip(tensor, d, n_t) + odd * flip(tensor, swapped(d, n_t), n_t)
        for d in range(1, n_t)
    ]
    sources = [
        t_peers[d - 1]
        if d % 2 == 0
        else (1 - odd) * flip(tensor, swapped(d, n_t), n_t) + odd * flip(tensor, d, n_t)
        for d in range(1, n_t)
    ]
    g_peers = [flip(group, d, n_g) for d in range(1, n_g)]
    barrier = pltpu.get_barrier_semaphore()
    for peer in t_peers:
        pl.semaphore_signal(barrier, inc=1, device_id={"tensor": peer}, device_id_type=MESH)
    for peer in g_peers:
        pl.semaphore_signal(barrier, inc=1, device_id={"group": peer}, device_id_type=MESH)
    for copy in small:
        copy.start()
    pl.semaphore_wait(barrier, n_t + n_g - 2)
    load.wait()

    def block(begin, count, d, send, recv):
        peer = t_peers[d - 1]
        return pltpu.make_async_remote_copy(
            src_ref=cache_v.at[pl.ds(begin, count), pl.ds(peer * span, span), :],
            dst_ref=arrived.at[pl.ds(tensor * pairs + begin, count)],
            send_sem=send.at[d],
            recv_sem=recv.at[d],
            device_id={"tensor": peer},
            device_id_type=MESH,
        )

    hops = {d: bin(d // 2).count("1") for d in range(1, n_t)}
    order = sorted(range(1, n_t), key=lambda d: (hops[d], d % 2, d))
    near = [d for d in order if hops[d] == 1]
    early = [(block(0, first, d, a_send_sem, a_recv_sem), d, 0, first) for d in near]
    for copy, *_ in early:
        copy.start()
    for e in range(experts):
        pltpu.make_async_copy(gate_hbm.at[e], gate_v.at[e], gate_sem.at[e]).start()
        pltpu.make_async_copy(up_hbm.at[e], up_v.at[e], up_sem.at[e]).start()
    for copy in small:
        copy.wait()

    begin = tensor * pairs
    seq = begin // kv_heads
    head0 = begin % kv_heads
    share = tensor % shares
    scale = 1.0 / math.sqrt(head)
    q = queries_ref[seq]
    fresh = fresh_ref[seq]
    length = lengths_ref[seq]
    row = lax.broadcasted_iota(jnp.int32, (q_heads, 1), 0)
    mine = [
        (row >= (head0 + p) * per) & (row < (head0 + p + 1) * per) for p in range(pairs)
    ]
    scores = jnp.zeros((q_heads, slots), jnp.float32)
    for p in range(pairs):
        s = lax.dot_general(q, cache_v[p, :, :head], NT, preferred_element_type=jnp.float32)
        scores = jnp.where(mine[p], s, scores)
    scores = scores * scale
    own_all = lax.dot_general(q, fresh[:, :head], NT, preferred_element_type=jnp.float32) * scale
    wide_row = lax.broadcasted_iota(jnp.int32, (q_heads, kv_heads), 0)
    wide_col = lax.broadcasted_iota(jnp.int32, (q_heads, kv_heads), 1)
    own_mask = (wide_row >= wide_col * per) & (wide_row < (wide_col + 1) * per)
    own_score = jnp.sum(jnp.where(own_mask, own_all, 0.0), axis=1, keepdims=True)
    visible = lax.broadcasted_iota(jnp.int32, (q_heads, slots), 1) < length
    scores = jnp.where(visible, scores, -1e30)
    peak = jnp.maximum(jnp.max(scores, axis=1, keepdims=True), own_score)
    weights = jnp.where(visible, jnp.exp(scores - peak), 0.0)
    own_weight = jnp.exp(own_score - peak)
    denominator = jnp.sum(weights, axis=1, keepdims=True) + own_weight
    rounded = weights.astype(jnp.bfloat16)
    own_rounded = jnp.where(own_mask, own_weight, 0.0).astype(jnp.bfloat16)
    own_value = jnp.dot(own_rounded, fresh[:, head:], preferred_element_type=jnp.float32)
    result = jnp.zeros((q_heads, head), jnp.float32)
    for p in range(pairs):
        o = jnp.dot(rounded, cache_v[p, :, head:], preferred_element_type=jnp.float32)
        result = jnp.where(mine[p], (o + own_value) / denominator, result)
    heads_b[seq, share] = result.astype(jnp.bfloat16)

    h_copies = []
    for d in order:
        copy = pltpu.make_async_remote_copy(
            src_ref=heads_b.at[seq, share],
            dst_ref=heads_b.at[seq, share],
            send_sem=h_send_sem.at[d],
            recv_sem=h_recv_sem.at[d],
            device_id={"tensor": t_peers[d - 1]},
            device_id_type=MESH,
        )
        copy.start()
        h_copies.append(copy)
    late = []
    if first < pairs:
        rest = pairs - first
        late = [(block(first, rest, d, b_send_sem, b_recv_sem), d, first, rest) for d in near]
    late += [
        (block(0, pairs, d, a_send_sem, a_recv_sem), d, 0, pairs) for d in order if hops[d] != 1
    ]
    for copy, *_ in late:
        copy.start()
    landings = early + late
    picked[...] = jnp.zeros_like(picked)
    lane = lax.broadcasted_iota(jnp.int32, (seqs, LANES), 1)
    diagonal = lax.broadcasted_iota(jnp.int32, (seqs, seqs), 0) == lax.broadcasted_iota(
        jnp.int32, (seqs, seqs), 1
    )
    ids = [
        jnp.sum(
            jnp.where(diagonal, routing_ref[k : k + 1, :].astype(jnp.float32), 0.0),
            axis=1,
            keepdims=True,
        )
        for k in range(2)
    ]
    tags = jnp.where(lane == 0, ids[0], jnp.where(lane == 1, ids[1], 0.0)).astype(jnp.bfloat16)
    for g in range(n_g):
        x_send[g, :, depth:] = tags
    for copy in h_copies:
        copy.wait_recv()

    heads_v[...] = heads_b[...].astype(jnp.float32)

    squares = jnp.zeros((seqs, LANES), jnp.float32)
    for c in range(0, columns, LANES):
        add = heads_v[:, 0, c // LANES, :]
        for other in range(1, shares):
            add = add + heads_v[:, other, c // LANES, :]
        u = (residual_ref[:, c : c + LANES].astype(jnp.float32) + add).astype(jnp.bfloat16)
        updated_ref[:, c : c + LANES] = u
        u = u.astype(jnp.float32)
        squares = squares + u * u
    factor = lax.rsqrt(jnp.sum(squares, axis=1, keepdims=True) / columns + 1e-05)
    for c in range(0, columns, LANES):
        u = updated_ref[:, c : c + LANES].astype(jnp.float32)
        n = (u * factor * gain_ref[:, c : c + LANES]).astype(jnp.bfloat16)
        normed_v[:, c : c + LANES] = n
        x_send[c // depth, :, c % depth : c % depth + LANES] = n
    x_copies = []
    for d in range(1, n_g):
        copy = pltpu.make_async_remote_copy(
            src_ref=x_send.at[g_peers[d - 1]],
            dst_ref=x_recv.at[group],
            send_sem=x_send_sem.at[d],
            recv_sem=x_recv_sem.at[d],
            device_id={"group": g_peers[d - 1]},
            device_id_type=MESH,
        )
        copy.start()
        x_copies.append(copy)
    x_recv[group] = x_send[group]
    logits = lax.dot_general(
        normed_v[...], router_ref[...], NT, preferred_element_type=jnp.float32
    )
    expert_col = lax.broadcasted_iota(jnp.int32, (seqs, experts), 1)
    chosen = [
        jnp.sum(jnp.where(expert_col == ids[k].astype(jnp.int32), logits, 0.0), axis=1, keepdims=True)
        for k in range(2)
    ]
    gap = chosen[0] - chosen[1]
    gates = [jax.nn.sigmoid(gap), jax.nn.sigmoid(-gap)]
    for copy in x_copies:
        copy.wait_recv()

    parts = [x_recv[g].astype(jnp.float32) for g in range(n_g)]
    tokens = jnp.concatenate(parts, axis=0)
    x = tokens[:, :depth].astype(jnp.bfloat16)
    tag = tokens[:, depth:]

    def expert(e, carry):
        picks = [tag[:, k : k + 1] == e.astype(jnp.float32) for k in range(2)]
        for which, (hbm, buf, sem) in enumerate(
            ((gate_hbm, gate_v, gate_sem), (up_hbm, up_v, up_sem))
        ):
            pltpu.make_async_copy(hbm.at[e], buf.at[e], sem.at[e]).wait()
            part = jnp.dot(x, buf[e], preferred_element_type=jnp.float32)
            for k in range(2):
                picked[k, which] = jnp.where(picks[k], part, picked[k, which])
        return carry

    lax.fori_loop(0, experts, expert, 0)

    for g in range(n_g):
        p_send[g] = picked[:, :, g * seqs : (g + 1) * seqs, :].astype(jnp.bfloat16)
    p_copies = []
    for d in range(1, n_g):
        copy = pltpu.make_async_remote_copy(
            src_ref=p_send.at[g_peers[d - 1]],
            dst_ref=p_recv.at[group],
            send_sem=p_send_sem.at[d],
            recv_sem=p_recv_sem.at[d],
            device_id={"group": g_peers[d - 1]},
            device_id_type=MESH,
        )
        copy.start()
        p_copies.append(copy)
    p_recv[group] = p_send[group]
    for copy in p_copies:
        copy.wait_recv()
    values = []
    for k in range(2):
        sums = []
        for which in range(2):
            total = p_recv[0, k, which].astype(jnp.float32)
            for g in range(1, n_g):
                total = total + p_recv[g, k, which].astype(jnp.float32)
            sums.append(total)
        values.append(gates[k] * (sums[0] / (1.0 + jnp.exp(-sums[0]))) * sums[1])
    hidden_ref[...] = jnp.stack(values, axis=1).astype(jnp.bfloat16)

    fresh_rows[...] = fresh_ref[...].astype(jnp.float32).reshape(fresh_rows.shape)
    slot = lax.broadcasted_iota(jnp.int32, (span, width), 0).astype(jnp.float32).astype(jnp.bfloat16)

    def patch(source, begin, count):
        row = source * pairs + begin
        owner = row // kv_heads
        local = (lengths_ref[owner] - tensor * span).astype(jnp.float32).astype(jnp.bfloat16)
        here = slot == local
        for p in range(count):
            new = fresh_rows[pl.ds(row + p, 1), :].astype(jnp.bfloat16)
            yield p, row + p, here, new

    for p, at, here, new in patch(tensor, 0, pairs):
        arrived[at] = jnp.where(here, new, cache_v[p, pl.ds(tensor * span, span), :])
    for copy in h_copies + x_copies + p_copies:
        copy.wait_send()
    for copy, d, begin, count in landings:
        copy.wait_recv()
        for p, at, here, new in patch(sources[d - 1], begin, count):
            arrived[at] = jnp.where(here, new, arrived[at])
    for copy, d, begin, count in landings:
        copy.wait_send()


def finish(updated, hidden, arrived, updated_out, hidden_out, cache_out, sem):
    copies = [
        pltpu.make_async_copy(arrived, cache_out, sem.at[0]),
        pltpu.make_async_copy(updated, updated_out, sem.at[1]),
        pltpu.make_async_copy(hidden, hidden_out, sem.at[2]),
    ]
    for copy in copies:
        copy.start()
    for copy in copies:
        copy.wait()


def body(
    n_t,
    n_g,
    key_value_cache,
    queries,
    fresh_key_value,
    lengths,
    residual,
    norm_gain,
    router_weight,
    routing,
    expert_gate,
    expert_up,
):
    pairs, slots, width = key_value_cache.shape
    seqs, q_heads, head = queries.shape
    kv_heads = fresh_key_value.shape[1]
    columns = residual.shape[1]
    experts, depth, units = expert_gate.shape
    span = slots // n_t
    shares = kv_heads // pairs
    bf16, f32 = jnp.bfloat16, jnp.float32
    hbm = pl.BlockSpec(memory_space=pltpu.HBM)
    vmem = pl.BlockSpec(memory_space=pltpu.VMEM)
    dma = pltpu.SemaphoreType.DMA
    rows = n_t * pairs
    updated, hidden, arrived = pl.pallas_call(
        functools.partial(kernel, n_t, n_g),
        out_shape=(
            pltpu.VMEM((seqs, columns), bf16),
            pltpu.VMEM((seqs, 2, units), bf16),
            pltpu.VMEM((rows, span, width), bf16),
        ),
        in_specs=[hbm] * 10,
        out_specs=(vmem, vmem, vmem),
        scratch_shapes=[
            pltpu.VMEM((pairs, slots, width), bf16),
            pltpu.VMEM(queries.shape, bf16),
            pltpu.VMEM(fresh_key_value.shape, bf16),
            pltpu.VMEM((rows, width), f32),
            pltpu.SMEM(lengths.shape, jnp.int32),
            pltpu.VMEM(residual.shape, bf16),
            pltpu.VMEM((1, columns), f32),
            pltpu.VMEM((experts, columns), bf16),
            pltpu.VMEM((2, seqs), jnp.int32),
            pltpu.VMEM((experts, depth, units), bf16),
            pltpu.VMEM((experts, depth, units), bf16),
            pltpu.VMEM((seqs, shares, q_heads, head), bf16),
            pltpu.VMEM((seqs, shares, q_heads, head), f32),
            pltpu.VMEM((seqs, columns), bf16),
            pltpu.VMEM((n_g, seqs, depth + LANES), bf16),
            pltpu.VMEM((n_g, seqs, depth + LANES), bf16),
            pltpu.VMEM((2, 2, n_g * seqs, units), f32),
            pltpu.VMEM((n_g, 2, 2, seqs, units), bf16),
            pltpu.VMEM((n_g, 2, 2, seqs, units), bf16),
            dma,
            dma((7,)),
            dma((experts,)),
            dma((experts,)),
            dma((n_t,)),
            dma((n_t,)),
            dma((n_t,)),
            dma((n_t,)),
            dma((n_t,)),
            dma((n_t,)),
            dma((n_g,)),
            dma((n_g,)),
            dma((n_g,)),
            dma((n_g,)),
        ],
        compiler_params=pltpu.CompilerParams(
            collective_id=0, has_side_effects=True, vmem_limit_bytes=57 * 1024 * 1024
        ),
        name="decode_step",
    )(
        key_value_cache,
        queries,
        fresh_key_value,
        lengths,
        residual,
        norm_gain.reshape(1, columns),
        router_weight.T,
        routing.T,
        expert_gate,
        expert_up,
    )
    updated, hidden, new_cache = pl.pallas_call(
        finish,
        out_shape=(
            jax.ShapeDtypeStruct(updated.shape, bf16),
            jax.ShapeDtypeStruct(hidden.shape, bf16),
            jax.ShapeDtypeStruct(arrived.shape, bf16),
        ),
        in_specs=[vmem] * 3,
        out_specs=[hbm] * 3,
        scratch_shapes=[dma((3,))],
        compiler_params=pltpu.CompilerParams(vmem_limit_bytes=1024 * 1024),
        name="hand_over",
    )(*(pltpu.with_memory_space_constraint(x, pltpu.VMEM) for x in (updated, hidden, arrived)))
    return updated, hidden, new_cache.reshape(seqs, kv_heads, span, width)


def solution(mesh):
    in_specs = (
        P(("group", "tensor"), None, None),
        P("group", None, None),
        P("group", None, None),
        P("group"),
        P("group", None),
        P(),
        P(),
        P("group", None),
        P(None, "group", "tensor"),
        P(None, "group", "tensor"),
    )
    out_specs = (P("group", None), P("group", None, "tensor"), P("group", None, "tensor", None))
    step = functools.partial(body, mesh.shape["tensor"], mesh.shape["group"])
    return jax.shard_map(step, mesh=mesh, in_specs=in_specs, out_specs=out_specs, check_vma=False)
```

```python
import functools
import math

import jax
import jax.numpy as jnp
from jax import lax
from jax.experimental import pallas as pl
from jax.experimental.pallas import tpu as pltpu
from jax.sharding import PartitionSpec as P

MESH = pl.DeviceIdType.MESH
LANES = 128
NT = (((1,), (1,)), ((), ()))


def flip(rank, bits, count):
    out, step = rank, 1
    while step < count:
        if bits & step:
            out = out + step * (1 - 2 * (rank // step % 2))
        step *= 2
    return out


def swapped(bits, count):
    if count < 8 or (bits >> 1) % 2 == (bits >> 2) % 2:
        return bits
    return bits ^ 6


class enter:
    def __init__(self, n_t, n_g, tensor, group, t_peers, g_peers, go_sem, far_sem, z_sem):
        self.barrier = pltpu.get_barrier_semaphore()
        self.relayed = n_t == 8
        self.tensor, self.n_t, self.n_g = tensor, n_t, n_g
        self.t_peers, self.g_peers = t_peers, g_peers
        self.sems = go_sem, far_sem, z_sem
        self.lead = tensor % 2 == 1
        if not self.relayed:
            for peer in t_peers:
                self.signal(self.barrier, {"tensor": peer})
            for peer in g_peers:
                self.signal(self.barrier, {"group": peer})
            return
        base = tensor - tensor % 2 + 1
        for bits in (2, 4):
            self.signal(self.barrier, {"tensor": flip(base, bits, n_t)})

        @pl.when(jnp.logical_not(self.lead))
        def _():
            self.signal(self.barrier, {"tensor": base})

    def signal(self, sem, peer):
        pl.semaphore_signal(sem, inc=1, device_id=peer, device_id_type=MESH)

    def near(self):
        if not self.relayed:
            pl.semaphore_wait(self.barrier, self.n_t + self.n_g - 2)
            return
        go_sem, far_sem, _ = self.sems
        mate = flip(self.tensor, 1, self.n_t)

        @pl.when(self.lead)
        def _():
            pl.semaphore_wait(self.barrier, 5)
            self.signal(go_sem, {"tensor": mate})
            for bits in (2, 3):
                self.signal(far_sem, {"tensor": flip(self.tensor, bits, self.n_t)})

        @pl.when(jnp.logical_not(self.lead))
        def _():
            pl.semaphore_wait(go_sem, 1)

    def relay(self):
        if self.relayed:

            @pl.when(jnp.logical_not(self.lead))
            def _():
                for peer in self.g_peers:
                    self.signal(self.barrier, {"group": peer})

    def distant(self):
        if self.relayed:
            pl.semaphore_wait(self.sems[1], 1)

    def groups(self):
        if not self.relayed:
            return
        z_sem = self.sems[2]
        mate = flip(self.tensor, 1, self.n_t)

        @pl.when(jnp.logical_not(self.lead))
        def _():
            pl.semaphore_wait(self.barrier, self.n_g - 1)
            self.signal(z_sem, {"tensor": mate})

        @pl.when(self.lead)
        def _():
            pl.semaphore_wait(z_sem, 1)


def kernel(
    n_t,
    n_g,
    cache_hbm,
    queries_hbm,
    fresh_hbm,
    lengths_hbm,
    residual_hbm,
    gain_hbm,
    router_hbm,
    routing_hbm,
    gate_hbm,
    up_hbm,
    updated_ref,
    hidden_ref,
    arrived,
    cache_v,
    queries_ref,
    fresh_ref,
    fresh_rows,
    lengths_ref,
    residual_ref,
    gain_ref,
    router_ref,
    routing_ref,
    gate_v,
    up_v,
    heads_b,
    heads_v,
    normed_v,
    x_send,
    x_recv,
    picked,
    p_send,
    p_recv,
    load_sem,
    small_sem,
    gate_sem,
    up_sem,
    a_send_sem,
    a_recv_sem,
    b_send_sem,
    b_recv_sem,
    c_send_sem,
    c_recv_sem,
    h_send_sem,
    h_recv_sem,
    x_send_sem,
    x_recv_sem,
    p_send_sem,
    p_recv_sem,
    go_sem,
    far_sem,
    z_sem,
):
    tensor = lax.axis_index("tensor")
    group = lax.axis_index("group")
    pairs, slots, width = cache_v.shape
    head = width // 2
    span = slots // n_t
    cut = max(1, 3 * pairs // 8)
    later = max(cut, 5 * pairs // 8)
    seqs = residual_ref.shape[0]
    q_heads = queries_ref.shape[0]
    kv_heads = fresh_ref.shape[0]
    per = q_heads // kv_heads
    experts = gate_v.shape[0]
    depth = gate_v.shape[1]
    columns = residual_ref.shape[1]
    shares = heads_v.shape[1]

    begin = tensor * pairs
    seq = begin // kv_heads
    head0 = begin % kv_heads
    share = tensor % shares
    odd = tensor % 2
    t_peers = [
        (1 - odd) * flip(tensor, d, n_t) + odd * flip(tensor, swapped(d, n_t), n_t)
        for d in range(1, n_t)
    ]
    g_peers = [flip(group, d, n_g) for d in range(1, n_g)]
    hops = {d: bin(d // 2).count("1") for d in range(1, n_t)}
    order = sorted(range(1, n_t), key=lambda d: (hops[d], d % 2, d))
    near = [d for d in order if hops[d] == 1]
    far = [d for d in order if hops[d] > 1]
    small = [
        pltpu.make_async_copy(src, dst, small_sem.at[i])
        for i, (src, dst) in enumerate(
            (
                (lengths_hbm, lengths_ref),
                (fresh_hbm.at[seq], fresh_ref),
                (queries_hbm.at[seq], queries_ref),
                (routing_hbm, routing_ref),
                (residual_hbm, residual_ref),
                (gain_hbm, gain_ref),
                (router_hbm, router_ref),
            )
        )
    ]

    def slab(peer):
        return pl.ds(pl.multiple_of(peer * span, span), span)

    def fetch(d, first_row, count):
        peer = tensor if d == 0 else t_peers[d - 1]
        rows = pl.ds(first_row, count), slab(peer)
        at = d if first_row == 0 else n_t + d
        return pltpu.make_async_copy(cache_hbm.at[rows], cache_v.at[rows], load_sem.at[at])

    greet = enter(n_t, n_g, tensor, group, t_peers, g_peers, go_sem, far_sem, z_sem)
    loads = [fetch(d, 0, cut) for d in near]
    more = [fetch(d, cut, pairs - cut) for d in near if cut < pairs]
    more += [fetch(d, 0, pairs) for d in far + [1, 0]]
    small[0].start()
    small[1].start()
    for copy in loads + more:
        copy.start()
    for copy in small[2:]:
        copy.start()

    def block(first_row, count, d, send, recv):
        peer = t_peers[d - 1]
        return pltpu.make_async_remote_copy(
            src_ref=cache_v.at[pl.ds(first_row, count), slab(peer), :],
            dst_ref=arrived.at[pl.ds(begin + first_row, count)],
            send_sem=send.at[d],
            recv_sem=recv.at[d],
            device_id={"tensor": peer},
            device_id_type=MESH,
        )

    slot = lax.broadcasted_iota(jnp.int32, (span, width), 0).astype(jnp.float32)
    slot = slot.astype(jnp.bfloat16)
    small[0].wait()
    small[1].wait()
    length = lengths_ref[seq]
    fresh_rows[...] = fresh_ref[...].astype(jnp.float32)

    def patched(peer, p):
        here = slot == (length - peer * span).astype(jnp.float32).astype(jnp.bfloat16)
        new = fresh_rows[pl.ds(head0 + p, 1), :].astype(jnp.bfloat16)
        return jnp.where(here, new, cache_v[p, slab(peer), :])

    def patch(peer, first_row, count):
        for p in range(first_row, first_row + count):
            cache_v[p, slab(peer), :] = patched(peer, p)

    for d, copy in zip(near, loads):
        copy.wait()
        patch(t_peers[d - 1], 0, cut)
    greet.near()
    early = [block(0, cut, d, a_send_sem, a_recv_sem) for d in near]
    for copy in early:
        copy.start()
    greet.relay()
    for e in range(experts):
        pltpu.make_async_copy(gate_hbm.at[e], gate_v.at[e], gate_sem.at[e]).start()
        pltpu.make_async_copy(up_hbm.at[e], up_v.at[e], up_sem.at[e]).start()
    for copy in more:
        copy.wait()
    for copy in small[2:]:
        copy.wait()

    scale = 1.0 / math.sqrt(head)
    q = queries_ref[...]
    fresh = fresh_ref[...]
    row = lax.broadcasted_iota(jnp.int32, (q_heads, 1), 0)
    mine = [
        (row >= (head0 + p) * per) & (row < (head0 + p + 1) * per) for p in range(pairs)
    ]
    scores = jnp.zeros((q_heads, slots), jnp.float32)
    for p in range(pairs):
        s = lax.dot_general(q, cache_v[p, :, :head], NT, preferred_element_type=jnp.float32)
        scores = jnp.where(mine[p], s, scores)
    scores = scores * scale
    own_all = lax.dot_general(q, fresh[:, :head], NT, preferred_element_type=jnp.float32) * scale
    wide_row = lax.broadcasted_iota(jnp.int32, (q_heads, kv_heads), 0)
    wide_col = lax.broadcasted_iota(jnp.int32, (q_heads, kv_heads), 1)
    own_mask = (wide_row >= wide_col * per) & (wide_row < (wide_col + 1) * per)
    own_score = jnp.sum(jnp.where(own_mask, own_all, 0.0), axis=1, keepdims=True)
    visible = lax.broadcasted_iota(jnp.int32, (q_heads, slots), 1) < length
    scores = jnp.where(visible, scores, -1e30)
    peak = jnp.maximum(jnp.max(scores, axis=1, keepdims=True), own_score)
    weights = jnp.where(visible, jnp.exp(scores - peak), 0.0)
    own_weight = jnp.exp(own_score - peak)
    denominator = jnp.sum(weights, axis=1, keepdims=True) + own_weight
    rounded = weights.astype(jnp.bfloat16)
    own_rounded = jnp.where(own_mask, own_weight, 0.0).astype(jnp.bfloat16)
    own_value = jnp.dot(own_rounded, fresh[:, head:], preferred_element_type=jnp.float32)
    result = jnp.zeros((q_heads, head), jnp.float32)
    for p in range(pairs):
        o = jnp.dot(rounded, cache_v[p, :, head:], preferred_element_type=jnp.float32)
        result = jnp.where(mine[p], (o + own_value) / denominator, result)
    heads_b[seq, share] = result.astype(jnp.bfloat16)

    def pass_heads(owner, d, peer):
        at = owner * pairs // kv_heads, owner % shares
        return pltpu.make_async_remote_copy(
            src_ref=heads_b.at[at],
            dst_ref=heads_b.at[at],
            send_sem=h_send_sem.at[d],
            recv_sem=h_recv_sem.at[d],
            device_id={"tensor": peer},
            device_id_type=MESH,
        )

    greet.distant()
    mate = t_peers[0]
    same = [d for d in order if d % 2 == 0]
    h_copies = {d: pass_heads(tensor, d, t_peers[d - 1]) for d in same + [1]}
    for copy in h_copies.values():
        copy.start()
    for d in near:
        patch(t_peers[d - 1], cut, later - cut)
    patch(mate, 0, pairs)
    middle = [block(0, pairs, 1, a_send_sem, a_recv_sem)]
    if cut < later:
        middle += [block(cut, later - cut, d, c_send_sem, c_recv_sem) for d in near]
    for copy in middle:
        copy.start()
    for d in far:
        patch(t_peers[d - 1], 0, pairs)
    for d in near:
        patch(t_peers[d - 1], later, pairs - later)
    for p in range(pairs):
        arrived[begin + p] = patched(tensor, p)
    picked[...] = jnp.zeros_like(picked)
    lane = lax.broadcasted_iota(jnp.int32, (seqs, LANES), 1)
    diagonal = lax.broadcasted_iota(jnp.int32, (seqs, seqs), 0) == lax.broadcasted_iota(
        jnp.int32, (seqs, seqs), 1
    )
    ids = [
        jnp.sum(
            jnp.where(diagonal, routing_ref[k : k + 1, :].astype(jnp.float32), 0.0),
            axis=1,
            keepdims=True,
        )
        for k in range(2)
    ]
    tags = jnp.where(lane == 0, ids[0], jnp.where(lane == 1, ids[1], 0.0)).astype(jnp.bfloat16)
    for g in range(n_g):
        x_send[g, :, depth:] = tags
    for d in same:
        h_copies[d].wait_recv()
        h_copies[d + 1] = pass_heads(t_peers[d - 1], d + 1, mate)
        h_copies[d + 1].start()
    late = [block(0, pairs, d, a_send_sem, a_recv_sem) for d in far]
    if later < pairs:
        late += [block(later, pairs - later, d, b_send_sem, b_recv_sem) for d in near]
    for copy in late:
        copy.start()
    h_copies[1].wait_recv()
    for d in same:
        h_copies[d + 1].wait_recv()

    heads_v[...] = heads_b[...].astype(jnp.float32)

    squares = jnp.zeros((seqs, LANES), jnp.float32)
    for c in range(0, columns, LANES):
        add = heads_v[:, 0, c // LANES, :]
        for other in range(1, shares):
            add = add + heads_v[:, other, c // LANES, :]
        u = (residual_ref[:, c : c + LANES].astype(jnp.float32) + add).astype(jnp.bfloat16)
        updated_ref[:, c : c + LANES] = u
        u = u.astype(jnp.float32)
        squares = squares + u * u
    factor = lax.rsqrt(jnp.sum(squares, axis=1, keepdims=True) / columns + 1e-05)
    for c in range(0, columns, LANES):
        u = updated_ref[:, c : c + LANES].astype(jnp.float32)
        n = (u * factor * gain_ref[:, c : c + LANES]).astype(jnp.bfloat16)
        normed_v[:, c : c + LANES] = n
        x_send[c // depth, :, c % depth : c % depth + LANES] = n
    greet.groups()
    x_copies = []
    for d in range(1, n_g):
        copy = pltpu.make_async_remote_copy(
            src_ref=x_send.at[g_peers[d - 1]],
            dst_ref=x_recv.at[group],
            send_sem=x_send_sem.at[d],
            recv_sem=x_recv_sem.at[d],
            device_id={"group": g_peers[d - 1]},
            device_id_type=MESH,
        )
        copy.start()
        x_copies.append(copy)
    x_recv[group] = x_send[group]
    logits = lax.dot_general(
        normed_v[...], router_ref[...], NT, preferred_element_type=jnp.float32
    )
    expert_col = lax.broadcasted_iota(jnp.int32, (seqs, experts), 1)
    chosen = [
        jnp.sum(jnp.where(expert_col == ids[k].astype(jnp.int32), logits, 0.0), axis=1, keepdims=True)
        for k in range(2)
    ]
    gap = chosen[0] - chosen[1]
    gates = [jax.nn.sigmoid(gap), jax.nn.sigmoid(-gap)]
    for copy in x_copies:
        copy.wait_recv()

    parts = [x_recv[g].astype(jnp.float32) for g in range(n_g)]
    tokens = jnp.concatenate(parts, axis=0)
    x = tokens[:, :depth].astype(jnp.bfloat16)
    tag = tokens[:, depth:]

    def expert(e, carry):
        picks = [tag[:, k : k + 1] == e.astype(jnp.float32) for k in range(2)]
        for which, (hbm, buf, sem) in enumerate(
            ((gate_hbm, gate_v, gate_sem), (up_hbm, up_v, up_sem))
        ):
            pltpu.make_async_copy(hbm.at[e], buf.at[e], sem.at[e]).wait()
            part = jnp.dot(x, buf[e], preferred_element_type=jnp.float32)
            for k in range(2):
                picked[k, which] = jnp.where(picks[k], part, picked[k, which])
        return carry

    lax.fori_loop(0, experts, expert, 0)

    for g in range(n_g):
        p_send[g] = picked[:, :, g * seqs : (g + 1) * seqs, :].astype(jnp.bfloat16)
    p_copies = []
    for d in range(1, n_g):
        copy = pltpu.make_async_remote_copy(
            src_ref=p_send.at[g_peers[d - 1]],
            dst_ref=p_recv.at[group],
            send_sem=p_send_sem.at[d],
            recv_sem=p_recv_sem.at[d],
            device_id={"group": g_peers[d - 1]},
            device_id_type=MESH,
        )
        copy.start()
        p_copies.append(copy)
    p_recv[group] = p_send[group]
    for copy in p_copies:
        copy.wait_recv()
    values = []
    for k in range(2):
        sums = []
        for which in range(2):
            total = p_recv[0, k, which].astype(jnp.float32)
            for g in range(1, n_g):
                total = total + p_recv[g, k, which].astype(jnp.float32)
            sums.append(total)
        values.append(gates[k] * (sums[0] / (1.0 + jnp.exp(-sums[0]))) * sums[1])
    hidden_ref[...] = jnp.stack(values, axis=1).astype(jnp.bfloat16)

    for copy in list(h_copies.values()) + x_copies + p_copies:
        copy.wait_send()
    for copy in early + middle + late:
        copy.wait()


def finish(pieces, updated, hidden, arrived, updated_out, hidden_out, cache_out, sem):
    count = arrived.shape[0] // pieces
    copies = [
        pltpu.make_async_copy(
            arrived.at[pl.ds(i * count, count)], cache_out.at[pl.ds(i * count, count)], sem.at[i]
        )
        for i in range(pieces)
    ]
    copies.append(pltpu.make_async_copy(updated, updated_out, sem.at[pieces]))
    copies.append(pltpu.make_async_copy(hidden, hidden_out, sem.at[pieces + 1]))
    for copy in copies:
        copy.start()
    for copy in copies:
        copy.wait()


def body(
    n_t,
    n_g,
    key_value_cache,
    queries,
    fresh_key_value,
    lengths,
    residual,
    norm_gain,
    router_weight,
    routing,
    expert_gate,
    expert_up,
):
    pairs, slots, width = key_value_cache.shape
    seqs, q_heads, head = queries.shape
    kv_heads = fresh_key_value.shape[1]
    columns = residual.shape[1]
    experts, depth, units = expert_gate.shape
    span = slots // n_t
    shares = kv_heads // pairs
    bf16, f32 = jnp.bfloat16, jnp.float32
    hbm = pl.BlockSpec(memory_space=pltpu.HBM)
    vmem = pl.BlockSpec(memory_space=pltpu.VMEM)
    dma = pltpu.SemaphoreType.DMA
    regular = pltpu.SemaphoreType.REGULAR
    rows = n_t * pairs
    updated, hidden, arrived = pl.pallas_call(
        functools.partial(kernel, n_t, n_g),
        out_shape=(
            pltpu.VMEM((seqs, columns), bf16),
            pltpu.VMEM((seqs, 2, units), bf16),
            pltpu.VMEM((rows, span, width), bf16),
        ),
        in_specs=[hbm] * 10,
        out_specs=(vmem, vmem, vmem),
        scratch_shapes=[
            pltpu.VMEM((pairs, slots, width), bf16),
            pltpu.VMEM((q_heads, head), bf16),
            pltpu.VMEM((kv_heads, width), bf16),
            pltpu.VMEM((kv_heads, width), f32),
            pltpu.SMEM(lengths.shape, jnp.int32),
            pltpu.VMEM(residual.shape, bf16),
            pltpu.VMEM((1, columns), f32),
            pltpu.VMEM((experts, columns), bf16),
            pltpu.VMEM((2, seqs), jnp.int32),
            pltpu.VMEM((experts, depth, units), bf16),
            pltpu.VMEM((experts, depth, units), bf16),
            pltpu.VMEM((seqs, shares, q_heads, head), bf16),
            pltpu.VMEM((seqs, shares, q_heads, head), f32),
            pltpu.VMEM((seqs, columns), bf16),
            pltpu.VMEM((n_g, seqs, depth + LANES), bf16),
            pltpu.VMEM((n_g, seqs, depth + LANES), bf16),
            pltpu.VMEM((2, 2, n_g * seqs, units), f32),
            pltpu.VMEM((n_g, 2, 2, seqs, units), bf16),
            pltpu.VMEM((n_g, 2, 2, seqs, units), bf16),
            dma((2 * n_t,)),
            dma((7,)),
            dma((experts,)),
            dma((experts,)),
            dma((n_t,)),
            dma((n_t,)),
            dma((n_t,)),
            dma((n_t,)),
            dma((n_t,)),
            dma((n_t,)),
            dma((n_t,)),
            dma((n_t,)),
            dma((n_g,)),
            dma((n_g,)),
            dma((n_g,)),
            dma((n_g,)),
            regular,
            regular,
            regular,
        ],
        compiler_params=pltpu.CompilerParams(
            collective_id=0, has_side_effects=True, vmem_limit_bytes=57 * 1024 * 1024
        ),
        name="decode_step",
    )(
        key_value_cache,
        queries,
        fresh_key_value,
        lengths,
        residual,
        norm_gain.reshape(1, columns),
        router_weight.T,
        routing.T,
        expert_gate,
        expert_up,
    )
    updated, hidden, new_cache = pl.pallas_call(
        functools.partial(finish, 8),
        out_shape=(
            jax.ShapeDtypeStruct(updated.shape, bf16),
            jax.ShapeDtypeStruct(hidden.shape, bf16),
            jax.ShapeDtypeStruct(arrived.shape, bf16),
        ),
        in_specs=[vmem] * 3,
        out_specs=[hbm] * 3,
        scratch_shapes=[dma((10,))],
        compiler_params=pltpu.CompilerParams(vmem_limit_bytes=1024 * 1024),
        name="hand_over",
    )(*(pltpu.with_memory_space_constraint(x, pltpu.VMEM) for x in (updated, hidden, arrived)))
    return updated, hidden, new_cache.reshape(seqs, kv_heads, span, width)


def solution(mesh):
    in_specs = (
        P(("group", "tensor"), None, None),
        P("group", None, None),
        P("group", None, None),
        P("group"),
        P("group", None),
        P(),
        P(),
        P("group", None),
        P(None, "group", "tensor"),
        P(None, "group", "tensor"),
    )
    out_specs = (P("group", None), P("group", None, "tensor"), P("group", None, "tensor", None))
    step = functools.partial(body, mesh.shape["tensor"], mesh.shape["group"])
    return jax.shard_map(step, mesh=mesh, in_specs=in_specs, out_specs=out_specs, check_vma=False)
```

```python
import functools
import math

import jax
import jax.numpy as jnp
from jax import lax
from jax.experimental import pallas as pl
from jax.experimental.pallas import tpu as pltpu
from jax.sharding import PartitionSpec as P

MESH = pl.DeviceIdType.MESH
LANES = 128
NT = (((1,), (1,)), ((), ()))


def flip(rank, bits, count):
    out, step = rank, 1
    while step < count:
        if bits & step:
            out = out + step * (1 - 2 * (rank // step % 2))
        step *= 2
    return out


def swapped(bits, count):
    if count < 8 or (bits >> 1) % 2 == (bits >> 2) % 2:
        return bits
    return bits ^ 6


class enter:
    def __init__(self, n_t, n_g, tensor, t_peers, g_peers, *sems):
        self.barrier = pltpu.get_barrier_semaphore()
        self.relayed = n_t == 8
        self.tensor, self.n_t, self.n_g = tensor, n_t, n_g
        self.t_peers, self.g_peers = t_peers, g_peers
        self.sems = sems
        self.lead = tensor % 2 == 1
        if not self.relayed:
            for peer in t_peers:
                self.signal(self.barrier, {"tensor": peer})
            for peer in g_peers:
                self.signal(self.barrier, {"group": peer})
            return
        base = tensor - tensor % 2 + 1

        @pl.when(self.lead)
        def _():
            for bits in (2, 4):
                self.signal(self.barrier, {"tensor": flip(tensor, bits, n_t)})

        @pl.when(jnp.logical_not(self.lead))
        def _():
            self.signal(self.barrier, {"tensor": base})

    def signal(self, sem, peer):
        pl.semaphore_signal(sem, inc=1, device_id=peer, device_id_type=MESH)

    def near(self):
        if not self.relayed:
            pl.semaphore_wait(self.barrier, self.n_t + self.n_g - 2)
            return
        go_sem, pair_sem = self.sems[0], self.sems[3]

        @pl.when(self.lead)
        def _():
            pl.semaphore_wait(self.barrier, 3)
            for bits in (2, 4):
                self.signal(pair_sem, {"tensor": flip(self.tensor, bits, self.n_t)})

        @pl.when(jnp.logical_not(self.lead))
        def _():
            pl.semaphore_wait(go_sem, 1)

    def cross(self):
        if not self.relayed:
            return
        go_sem, far_sem, _, pair_sem = self.sems
        mate = flip(self.tensor, 1, self.n_t)

        @pl.when(self.lead)
        def _():
            pl.semaphore_wait(pair_sem, 2)
            self.signal(go_sem, {"tensor": mate})
            for bits in (2, 3):
                self.signal(far_sem, {"tensor": flip(self.tensor, bits, self.n_t)})

    def relay(self):
        if self.relayed:

            @pl.when(jnp.logical_not(self.lead))
            def _():
                for peer in self.g_peers:
                    self.signal(self.barrier, {"group": peer})

    def distant(self):
        if self.relayed:
            pl.semaphore_wait(self.sems[1], 1)

    def groups(self):
        if not self.relayed:
            return
        z_sem = self.sems[2]
        mate = flip(self.tensor, 1, self.n_t)

        @pl.when(jnp.logical_not(self.lead))
        def _():
            pl.semaphore_wait(self.barrier, self.n_g - 1)
            self.signal(z_sem, {"tensor": mate})

        @pl.when(self.lead)
        def _():
            pl.semaphore_wait(z_sem, 1)


def kernel(
    n_t,
    n_g,
    cache_hbm,
    queries_hbm,
    fresh_hbm,
    lengths_hbm,
    residual_hbm,
    gain_hbm,
    router_hbm,
    routing_hbm,
    gate_hbm,
    up_hbm,
    updated_ref,
    hidden_ref,
    arrived,
    cache_v,
    queries_ref,
    fresh_ref,
    fresh_rows,
    lengths_ref,
    residual_ref,
    gain_ref,
    router_ref,
    routing_ref,
    gate_v,
    up_v,
    heads_b,
    heads_v,
    normed_v,
    x_send,
    x_recv,
    picked,
    p_send,
    p_recv,
    load_sem,
    small_sem,
    gate_sem,
    up_sem,
    a_send_sem,
    a_recv_sem,
    b_send_sem,
    b_recv_sem,
    c_send_sem,
    c_recv_sem,
    h_send_sem,
    h_recv_sem,
    x_send_sem,
    x_recv_sem,
    p_send_sem,
    p_recv_sem,
    go_sem,
    far_sem,
    z_sem,
    pair_sem,
):
    tensor = lax.axis_index("tensor")
    group = lax.axis_index("group")
    pairs, slots, width = cache_v.shape
    head = width // 2
    span = slots // n_t
    cut = max(1, 3 * pairs // 8)
    later = max(cut, 5 * pairs // 8)
    seqs = residual_ref.shape[0]
    q_heads = queries_ref.shape[0]
    kv_heads = fresh_ref.shape[0]
    per = q_heads // kv_heads
    experts = gate_v.shape[0]
    depth = gate_v.shape[1]
    columns = residual_ref.shape[1]
    shares = heads_v.shape[1]

    begin = tensor * pairs
    seq = begin // kv_heads
    head0 = begin % kv_heads
    share = tensor % shares
    odd = tensor % 2
    t_peers = [
        (1 - odd) * flip(tensor, d, n_t) + odd * flip(tensor, swapped(d, n_t), n_t)
        for d in range(1, n_t)
    ]
    g_peers = [flip(group, d, n_g) for d in range(1, n_g)]
    hops = {d: bin(d // 2).count("1") for d in range(1, n_t)}
    order = sorted(range(1, n_t), key=lambda d: (hops[d], d % 2, d))
    near = [d for d in order if hops[d] == 1]
    far = [d for d in order if hops[d] > 1]
    small = [
        pltpu.make_async_copy(src, dst, small_sem.at[i])
        for i, (src, dst) in enumerate(
            (
                (lengths_hbm, lengths_ref),
                (fresh_hbm.at[seq], fresh_ref),
                (queries_hbm.at[seq], queries_ref),
                (routing_hbm, routing_ref),
                (residual_hbm, residual_ref),
                (gain_hbm, gain_ref),
                (router_hbm, router_ref),
            )
        )
    ]

    def slab(peer):
        return pl.ds(pl.multiple_of(peer * span, span), span)

    def fetch(d, first_row, count):
        peer = tensor if d == 0 else t_peers[d - 1]
        rows = pl.ds(first_row, count), slab(peer)
        at = d if first_row == 0 else n_t + d
        return pltpu.make_async_copy(cache_hbm.at[rows], cache_v.at[rows], load_sem.at[at])

    greet = enter(n_t, n_g, tensor, t_peers, g_peers, go_sem, far_sem, z_sem, pair_sem)
    loads = [fetch(d, 0, cut) for d in near]
    more = [fetch(d, cut, pairs - cut) for d in near if cut < pairs]
    more += [fetch(d, 0, pairs) for d in far + [1, 0]]
    small[0].start()
    small[1].start()
    for copy in loads + more:
        copy.start()
    for copy in small[2:]:
        copy.start()

    def block(first_row, count, d, send, recv):
        peer = t_peers[d - 1]
        return pltpu.make_async_remote_copy(
            src_ref=cache_v.at[pl.ds(first_row, count), slab(peer), :],
            dst_ref=arrived.at[pl.ds(begin + first_row, count)],
            send_sem=send.at[d],
            recv_sem=recv.at[d],
            device_id={"tensor": peer},
            device_id_type=MESH,
        )

    slot = lax.broadcasted_iota(jnp.int32, (span, width), 0).astype(jnp.float32)
    slot = slot.astype(jnp.bfloat16)
    small[0].wait()
    small[1].wait()
    length = lengths_ref[seq]
    fresh_rows[...] = fresh_ref[...].astype(jnp.float32)

    def patched(peer, p):
        here = slot == (length - peer * span).astype(jnp.float32).astype(jnp.bfloat16)
        new = fresh_rows[pl.ds(head0 + p, 1), :].astype(jnp.bfloat16)
        return jnp.where(here, new, cache_v[p, slab(peer), :])

    def patch(peer, first_row, count):
        for p in range(first_row, first_row + count):
            cache_v[p, slab(peer), :] = patched(peer, p)

    for d, copy in zip(near, loads):
        copy.wait()
        patch(t_peers[d - 1], 0, cut)
    greet.near()
    early = [block(0, cut, d, a_send_sem, a_recv_sem) for d in near]
    straight = sum(d % 2 == 0 for d in near)
    for copy in early[:straight]:
        copy.start()
    greet.cross()
    for copy in early[straight:]:
        copy.start()
    greet.relay()
    for e in range(experts):
        pltpu.make_async_copy(gate_hbm.at[e], gate_v.at[e], gate_sem.at[e]).start()
        pltpu.make_async_copy(up_hbm.at[e], up_v.at[e], up_sem.at[e]).start()
    for copy in more:
        copy.wait()
    for copy in small[2:]:
        copy.wait()

    scale = 1.0 / math.sqrt(head)
    q = queries_ref[...]
    fresh = fresh_ref[...]
    row = lax.broadcasted_iota(jnp.int32, (q_heads, 1), 0)
    mine = [
        (row >= (head0 + p) * per) & (row < (head0 + p + 1) * per) for p in range(pairs)
    ]
    scores = jnp.zeros((q_heads, slots), jnp.float32)
    for p in range(pairs):
        s = lax.dot_general(q, cache_v[p, :, :head], NT, preferred_element_type=jnp.float32)
        scores = jnp.where(mine[p], s, scores)
    scores = scores * scale
    own_all = lax.dot_general(q, fresh[:, :head], NT, preferred_element_type=jnp.float32) * scale
    wide_row = lax.broadcasted_iota(jnp.int32, (q_heads, kv_heads), 0)
    wide_col = lax.broadcasted_iota(jnp.int32, (q_heads, kv_heads), 1)
    own_mask = (wide_row >= wide_col * per) & (wide_row < (wide_col + 1) * per)
    own_score = jnp.sum(jnp.where(own_mask, own_all, 0.0), axis=1, keepdims=True)
    visible = lax.broadcasted_iota(jnp.int32, (q_heads, slots), 1) < length
    scores = jnp.where(visible, scores, -1e30)
    peak = jnp.maximum(jnp.max(scores, axis=1, keepdims=True), own_score)
    weights = jnp.where(visible, jnp.exp(scores - peak), 0.0)
    own_weight = jnp.exp(own_score - peak)
    denominator = jnp.sum(weights, axis=1, keepdims=True) + own_weight
    rounded = weights.astype(jnp.bfloat16)
    own_rounded = jnp.where(own_mask, own_weight, 0.0).astype(jnp.bfloat16)
    own_value = jnp.dot(own_rounded, fresh[:, head:], preferred_element_type=jnp.float32)
    result = jnp.zeros((q_heads, head), jnp.float32)
    for p in range(pairs):
        o = jnp.dot(rounded, cache_v[p, :, head:], preferred_element_type=jnp.float32)
        result = jnp.where(mine[p], (o + own_value) / denominator, result)
    heads_b[seq, share] = result.astype(jnp.bfloat16)

    def pass_heads(owner, d, peer):
        at = owner * pairs // kv_heads, owner % shares
        return pltpu.make_async_remote_copy(
            src_ref=heads_b.at[at],
            dst_ref=heads_b.at[at],
            send_sem=h_send_sem.at[d],
            recv_sem=h_recv_sem.at[d],
            device_id={"tensor": peer},
            device_id_type=MESH,
        )

    greet.distant()
    mate = t_peers[0]
    same = [d for d in order if d % 2 == 0]
    h_copies = {d: pass_heads(tensor, d, t_peers[d - 1]) for d in same + [1]}
    for copy in h_copies.values():
        copy.start()
    for d in near:
        patch(t_peers[d - 1], cut, later - cut)
    patch(mate, 0, pairs)
    middle = [block(0, pairs, 1, a_send_sem, a_recv_sem)]
    if cut < later:
        middle += [block(cut, later - cut, d, c_send_sem, c_recv_sem) for d in near]
    for copy in middle:
        copy.start()
    for d in far:
        patch(t_peers[d - 1], 0, pairs)
    for d in near:
        patch(t_peers[d - 1], later, pairs - later)
    for p in range(pairs):
        arrived[begin + p] = patched(tensor, p)
    picked[...] = jnp.zeros_like(picked)
    lane = lax.broadcasted_iota(jnp.int32, (seqs, LANES), 1)
    diagonal = lax.broadcasted_iota(jnp.int32, (seqs, seqs), 0) == lax.broadcasted_iota(
        jnp.int32, (seqs, seqs), 1
    )
    ids = [
        jnp.sum(
            jnp.where(diagonal, routing_ref[k : k + 1, :].astype(jnp.float32), 0.0),
            axis=1,
            keepdims=True,
        )
        for k in range(2)
    ]
    tags = jnp.where(lane == 0, ids[0], jnp.where(lane == 1, ids[1], 0.0)).astype(jnp.bfloat16)
    for g in range(n_g):
        x_send[g, :, depth:] = tags
    for d in same:
        h_copies[d].wait_recv()
        h_copies[d + 1] = pass_heads(t_peers[d - 1], d + 1, mate)
        h_copies[d + 1].start()
    late = [block(0, pairs, d, a_send_sem, a_recv_sem) for d in far]
    if later < pairs:
        late += [block(later, pairs - later, d, b_send_sem, b_recv_sem) for d in near]
    for copy in late:
        copy.start()
    h_copies[1].wait_recv()
    for d in same:
        h_copies[d + 1].wait_recv()

    heads_v[...] = heads_b[...].astype(jnp.float32)

    squares = jnp.zeros((seqs, LANES), jnp.float32)
    for c in range(0, columns, LANES):
        add = heads_v[:, 0, c // LANES, :]
        for other in range(1, shares):
            add = add + heads_v[:, other, c // LANES, :]
        u = (residual_ref[:, c : c + LANES].astype(jnp.float32) + add).astype(jnp.bfloat16)
        updated_ref[:, c : c + LANES] = u
        u = u.astype(jnp.float32)
        squares = squares + u * u
    factor = lax.rsqrt(jnp.sum(squares, axis=1, keepdims=True) / columns + 1e-05)
    for c in range(0, columns, LANES):
        u = updated_ref[:, c : c + LANES].astype(jnp.float32)
        n = (u * factor * gain_ref[:, c : c + LANES]).astype(jnp.bfloat16)
        normed_v[:, c : c + LANES] = n
        x_send[c // depth, :, c % depth : c % depth + LANES] = n
    greet.groups()
    x_copies = []
    for d in range(1, n_g):
        copy = pltpu.make_async_remote_copy(
            src_ref=x_send.at[g_peers[d - 1]],
            dst_ref=x_recv.at[group],
            send_sem=x_send_sem.at[d],
            recv_sem=x_recv_sem.at[d],
            device_id={"group": g_peers[d - 1]},
            device_id_type=MESH,
        )
        copy.start()
        x_copies.append(copy)
    x_recv[group] = x_send[group]
    logits = lax.dot_general(
        normed_v[...], router_ref[...], NT, preferred_element_type=jnp.float32
    )
    expert_col = lax.broadcasted_iota(jnp.int32, (seqs, experts), 1)
    chosen = [
        jnp.sum(jnp.where(expert_col == ids[k].astype(jnp.int32), logits, 0.0), axis=1, keepdims=True)
        for k in range(2)
    ]
    gap = chosen[0] - chosen[1]
    gates = [jax.nn.sigmoid(gap), jax.nn.sigmoid(-gap)]
    for copy in x_copies:
        copy.wait_recv()

    parts = [x_recv[g].astype(jnp.float32) for g in range(n_g)]
    tokens = jnp.concatenate(parts, axis=0)
    x = tokens[:, :depth].astype(jnp.bfloat16)
    tag = tokens[:, depth:]

    def expert(e, carry):
        picks = [tag[:, k : k + 1] == e.astype(jnp.float32) for k in range(2)]
        for which, (hbm, buf, sem) in enumerate(
            ((gate_hbm, gate_v, gate_sem), (up_hbm, up_v, up_sem))
        ):
            pltpu.make_async_copy(hbm.at[e], buf.at[e], sem.at[e]).wait()
            part = jnp.dot(x, buf[e], preferred_element_type=jnp.float32)
            for k in range(2):
                picked[k, which] = jnp.where(picks[k], part, picked[k, which])
        return carry

    lax.fori_loop(0, experts, expert, 0)

    for g in range(n_g):
        p_send[g] = picked[:, :, g * seqs : (g + 1) * seqs, :].astype(jnp.bfloat16)
    p_copies = []
    for d in range(1, n_g):
        copy = pltpu.make_async_remote_copy(
            src_ref=p_send.at[g_peers[d - 1]],
            dst_ref=p_recv.at[group],
            send_sem=p_send_sem.at[d],
            recv_sem=p_recv_sem.at[d],
            device_id={"group": g_peers[d - 1]},
            device_id_type=MESH,
        )
        copy.start()
        p_copies.append(copy)
    p_recv[group] = p_send[group]
    for copy in p_copies:
        copy.wait_recv()
    values = []
    for k in range(2):
        sums = []
        for which in range(2):
            total = p_recv[0, k, which].astype(jnp.float32)
            for g in range(1, n_g):
                total = total + p_recv[g, k, which].astype(jnp.float32)
            sums.append(total)
        values.append(gates[k] * (sums[0] / (1.0 + jnp.exp(-sums[0]))) * sums[1])
    hidden_ref[...] = jnp.stack(values, axis=1).astype(jnp.bfloat16)

    for copy in list(h_copies.values()) + x_copies + p_copies:
        copy.wait_send()
    for copy in early + middle + late:
        copy.wait()


def finish(pieces, updated, hidden, arrived, updated_out, hidden_out, cache_out, sem):
    count = arrived.shape[0] // pieces
    copies = [
        pltpu.make_async_copy(
            arrived.at[pl.ds(i * count, count)], cache_out.at[pl.ds(i * count, count)], sem.at[i]
        )
        for i in range(pieces)
    ]
    copies.append(pltpu.make_async_copy(updated, updated_out, sem.at[pieces]))
    copies.append(pltpu.make_async_copy(hidden, hidden_out, sem.at[pieces + 1]))
    for copy in copies:
        copy.start()
    for copy in copies:
        copy.wait()


def body(
    n_t,
    n_g,
    key_value_cache,
    queries,
    fresh_key_value,
    lengths,
    residual,
    norm_gain,
    router_weight,
    routing,
    expert_gate,
    expert_up,
):
    pairs, slots, width = key_value_cache.shape
    seqs, q_heads, head = queries.shape
    kv_heads = fresh_key_value.shape[1]
    columns = residual.shape[1]
    experts, depth, units = expert_gate.shape
    span = slots // n_t
    shares = kv_heads // pairs
    bf16, f32 = jnp.bfloat16, jnp.float32
    hbm = pl.BlockSpec(memory_space=pltpu.HBM)
    vmem = pl.BlockSpec(memory_space=pltpu.VMEM)
    dma = pltpu.SemaphoreType.DMA
    regular = pltpu.SemaphoreType.REGULAR
    rows = n_t * pairs
    updated, hidden, arrived = pl.pallas_call(
        functools.partial(kernel, n_t, n_g),
        out_shape=(
            pltpu.VMEM((seqs, columns), bf16),
            pltpu.VMEM((seqs, 2, units), bf16),
            pltpu.VMEM((rows, span, width), bf16),
        ),
        in_specs=[hbm] * 10,
        out_specs=(vmem, vmem, vmem),
        scratch_shapes=[
            pltpu.VMEM((pairs, slots, width), bf16),
            pltpu.VMEM((q_heads, head), bf16),
            pltpu.VMEM((kv_heads, width), bf16),
            pltpu.VMEM((kv_heads, width), f32),
            pltpu.SMEM(lengths.shape, jnp.int32),
            pltpu.VMEM(residual.shape, bf16),
            pltpu.VMEM((1, columns), f32),
            pltpu.VMEM((experts, columns), bf16),
            pltpu.VMEM((2, seqs), jnp.int32),
            pltpu.VMEM((experts, depth, units), bf16),
            pltpu.VMEM((experts, depth, units), bf16),
            pltpu.VMEM((seqs, shares, q_heads, head), bf16),
            pltpu.VMEM((seqs, shares, q_heads, head), f32),
            pltpu.VMEM((seqs, columns), bf16),
            pltpu.VMEM((n_g, seqs, depth + LANES), bf16),
            pltpu.VMEM((n_g, seqs, depth + LANES), bf16),
            pltpu.VMEM((2, 2, n_g * seqs, units), f32),
            pltpu.VMEM((n_g, 2, 2, seqs, units), bf16),
            pltpu.VMEM((n_g, 2, 2, seqs, units), bf16),
            dma((2 * n_t,)),
            dma((7,)),
            dma((experts,)),
            dma((experts,)),
            dma((n_t,)),
            dma((n_t,)),
            dma((n_t,)),
            dma((n_t,)),
            dma((n_t,)),
            dma((n_t,)),
            dma((n_t,)),
            dma((n_t,)),
            dma((n_g,)),
            dma((n_g,)),
            dma((n_g,)),
            dma((n_g,)),
            regular,
            regular,
            regular,
            regular,
        ],
        compiler_params=pltpu.CompilerParams(
            collective_id=0, has_side_effects=True, vmem_limit_bytes=57 * 1024 * 1024
        ),
        name="decode_step",
    )(
        key_value_cache,
        queries,
        fresh_key_value,
        lengths,
        residual,
        norm_gain.reshape(1, columns),
        router_weight.T,
        routing.T,
        expert_gate,
        expert_up,
    )
    updated, hidden, new_cache = pl.pallas_call(
        functools.partial(finish, 8),
        out_shape=(
            jax.ShapeDtypeStruct(updated.shape, bf16),
            jax.ShapeDtypeStruct(hidden.shape, bf16),
            jax.ShapeDtypeStruct(arrived.shape, bf16),
        ),
        in_specs=[vmem] * 3,
        out_specs=[hbm] * 3,
        scratch_shapes=[dma((10,))],
        compiler_params=pltpu.CompilerParams(vmem_limit_bytes=1024 * 1024),
        name="hand_over",
    )(*(pltpu.with_memory_space_constraint(x, pltpu.VMEM) for x in (updated, hidden, arrived)))
    return updated, hidden, new_cache.reshape(seqs, kv_heads, span, width)


def solution(mesh):
    in_specs = (
        P(("group", "tensor"), None, None),
        P("group", None, None),
        P("group", None, None),
        P("group"),
        P("group", None),
        P(),
        P(),
        P("group", None),
        P(None, "group", "tensor"),
        P(None, "group", "tensor"),
    )
    out_specs = (P("group", None), P("group", None, "tensor"), P("group", None, "tensor", None))
    step = functools.partial(body, mesh.shape["tensor"], mesh.shape["group"])
    return jax.shard_map(step, mesh=mesh, in_specs=in_specs, out_specs=out_specs, check_vma=False)
```
